64 devices in a mesh: prob: 4 (over x, y), feat: 16 (over z, core).
Axes of the slice: x: 2, y: 2, z: 8, core: 2. Of those that a mesh axis runs over, the one named last changes fastest.
The devices are a block of a 4x4x8 slice.
Arguments:
- design: bfloat16 [65536, 4096], P('prob', 'feat'), parts along dimension 0
- coef_init: float32 [16384, 6], P(('prob', 'feat')), parts along dimension 0
- targets: float32 [65536, 6], P('prob'), parts along dimension 0
- step_sizes: float32 [16384], P(('prob', 'feat')), parts along dimension 0
Outputs:
- output 1: float32 [16384, 6], P(('prob', 'feat')), parts along dimension 0
- output 2: float32 [65536, 6], P('prob'), parts along dimension 0
There are 4 independent parts. The reference program is written for one: setup_inputs(seed, part) draws one part's arguments, and reference() takes and returns one part's arrays. A program takes and returns all parts, laid end to end along the dimension named above; each array names one.
All inputs are finite; a program needn't handle non-finite values.
Results may differ from the reference program's by a relative error of at most 0.00481854.
Values are sent between devices in bfloat16 or wider.
A program may use at most 768 MiB of HBM per device.

```python
import jax
import jax.numpy as jnp
from jax import lax

SAMPLES = 16384
FEAT_DEV = 256
GROUP_SIZE = 16
TARGETS = 6
SWEEPS = 6
FACTORS = 4

FEATURES = FEAT_DEV * GROUP_SIZE
COMBINE_WEIGHT = 0.8
LASSO_WEIGHT = 0.3 * GROUP_SIZE / FEATURES ** 0.5


def setup_inputs(seed: int = 0, part: int = 0) -> dict:
    part_key = jax.random.fold_in(jax.random.key(seed), part)
    draw_keys = jax.random.split(part_key, 9)
    factor_rows = jax.random.normal(draw_keys[0], (SAMPLES, FACTORS), jnp.float32)
    loadings = jax.random.normal(draw_keys[1], (FACTORS, FEATURES), jnp.float32) * (0.5 / FEAT_DEV) ** 0.5

    def draw_block(block_index):
        noise_x = jax.random.normal(jax.random.fold_in(draw_keys[2], block_index), (SAMPLES, FEAT_DEV), jnp.float32)
        load_block = lax.dynamic_slice_in_dim(loadings, block_index * FEAT_DEV, FEAT_DEV, 1)
        x_block = (jnp.dot(factor_rows, load_block) + noise_x).astype(jnp.bfloat16)
        col_sq = jnp.sum(jnp.square(x_block.astype(jnp.float32)), axis=0)
        return x_block, col_sq

    x_blocks, col_sq = lax.map(draw_block, jnp.arange(GROUP_SIZE))
    design = jnp.transpose(x_blocks, (1, 0, 2)).reshape(SAMPLES, FEATURES)
    step_scale = jax.random.uniform(draw_keys[3], (FEATURES,), jnp.float32, 0.5, 1.0)
    step_sizes = step_scale * SAMPLES / (GROUP_SIZE * col_sq.reshape(FEATURES))
    support = jax.random.bernoulli(draw_keys[4], 0.125, (FEATURES, TARGETS)).astype(jnp.float32)
    true_weights = jax.random.normal(draw_keys[5], (FEATURES, TARGETS), jnp.float32) * support * (4.0 / FEATURES) ** 0.5
    factor_weights = jax.random.normal(draw_keys[6], (FACTORS, TARGETS), jnp.float32) * FACTORS ** -0.5
    noise_y = jax.random.normal(draw_keys[7], (SAMPLES, TARGETS), jnp.float32)
    signal = jnp.dot(design, true_weights.astype(jnp.bfloat16), preferred_element_type=jnp.float32)
    targets = jnp.dot(factor_rows, factor_weights) + signal + 0.5 * noise_y
    coef_init = jax.random.normal(draw_keys[8], (FEATURES, TARGETS), jnp.float32) * FEATURES ** -0.5
    return {'design': design, 'coef_init': coef_init, 'targets': targets, 'step_sizes': step_sizes}


def reference(design, coef_init, targets, step_sizes):
    x_blocks = jnp.transpose(design.reshape(SAMPLES, GROUP_SIZE, FEAT_DEV), (1, 0, 2))
    step_col = step_sizes[:, None]
    thresholds = step_col * LASSO_WEIGHT

    def block_sum(values):
        value_blocks = values.astype(jnp.bfloat16).reshape(GROUP_SIZE, FEAT_DEV, TARGETS)

        def add_block(running, operands):
            x_block, v_block = operands
            product = jnp.dot(x_block, v_block, preferred_element_type=jnp.float32).astype(jnp.bfloat16)
            return running + product.astype(jnp.float32), None

        running, _ = lax.scan(add_block, jnp.zeros((SAMPLES, TARGETS), jnp.float32), (x_blocks, value_blocks))
        return running

    residual = targets - block_sum(coef_init)

    def sweep(carry, _):
        weights, residual = carry
        gradient = lax.dot_general(design, residual.astype(jnp.bfloat16), (((0,), (0,)), ((), ())), preferred_element_type=jnp.float32) / SAMPLES
        stepped = weights + step_col * gradient
        shrunk = jnp.sign(stepped) * jnp.maximum(jnp.abs(stepped) - thresholds, 0.0)
        change = shrunk - weights
        weights = weights + COMBINE_WEIGHT * change
        residual = residual - COMBINE_WEIGHT * block_sum(change)
        return (weights, residual), None

    (weights, residual), _ = lax.scan(sweep, (coef_init, residual), None, length=SWEEPS)
    return (weights, residual)
```

```python
import functools

import jax
import jax.numpy as jnp
from jax import lax
from jax.experimental import pallas as pl
from jax.experimental.pallas import tpu as pltpu
from jax.sharding import PartitionSpec as P

SWEEPS = 6
COMBINE_WEIGHT = 0.8
LANES = 128
SUB = 8
MESH = pl.DeviceIdType.MESH
F32 = jnp.float32
BF16 = jnp.bfloat16


def ring_order(chips):
    order = [chips // 2]
    for d in range(chips // 2 - 1, 0, -1):
        order += [d, chips - d]
    return order + [0]


def kernel(group, lasso_weight, x_hbm, w0_ref, y_hbm, eta_ref, wt_ref, rt_ref,
           xv, yv, lbuf, usend, rs, ag, agf, rbuf, wbuf,
           x_sem, y_sem, rs_send, rs_recv, ag_send, ag_recv, fwd_send, fin_send, fin_recv, ffwd_send):
    chips = group // 2
    samples, width = xv.shape
    own = samples // group
    blocks = own // LANES
    targets = w0_ref.shape[0]
    rows = targets * SUB
    me = lax.axis_index('feat')
    chip = me // 2
    core = me % 2
    partner = chip * 2 + (1 - core)
    far_first = ring_order(chips)
    near_first = far_first[::-1]

    def chip_at(d):
        return (chip + d) % chips

    barrier = pltpu.get_barrier_semaphore()
    for k in range(1, group):
        pl.semaphore_signal(barrier, inc=1, device_id={'feat': (me + k) % group}, device_id_type=MESH)

    def x_copy(z, d):
        part = pl.ds(pl.multiple_of(z * (2 * own), 2 * own), 2 * own)
        return pltpu.make_async_copy(x_hbm.at[part, :], xv.at[part, :], x_sem.at[d])

    y_copy = pltpu.make_async_copy(y_hbm.at[:, pl.ds(pl.multiple_of(me * own, own), own)], yv, y_sem)
    for d in far_first:
        x_copy(chip_at(d), d).start()
    y_copy.start()

    row_id = lax.broadcasted_iota(jnp.int32, (rows, LANES), 0)
    sub_masks = [(row_id % SUB) == s for s in range(SUB)]

    def pick(value, s):
        wide = [jnp.where(sub_masks[s], value[:, i * LANES:(i + 1) * LANES], jnp.zeros((), value.dtype)) for i in range(value.shape[1] // LANES)]
        return wide[0] if len(wide) == 1 else jnp.concatenate(wide, axis=1)

    def fill_lhs(values):
        for s in range(SUB):
            lbuf[s] = pick(values, s).astype(BF16)

    def product(z):
        base = pl.multiple_of(z * (2 * own), 2 * own)
        total = None
        for s in range(blocks):
            first = xv[pl.ds(base + s * LANES, LANES), :]
            second = xv[pl.ds(base + own + s * LANES, LANES), :]
            part = lax.dot_general(lbuf[s], jnp.concatenate([first, second], axis=0), (((1,), (1,)), ((), ())), preferred_element_type=F32)
            total = part if total is None else total + part
        return total.astype(BF16)

    def rs_copy(dst):
        return pltpu.make_async_remote_copy(src_ref=usend.at[dst], dst_ref=rs.at[me], send_sem=rs_send.at[dst], recv_sem=rs_recv.at[me], device_id={'feat': dst}, device_id_type=MESH)

    def rs_arrival(src):
        return pltpu.make_async_remote_copy(src_ref=usend.at[src], dst_ref=rs.at[src], send_sem=rs_send.at[src], recv_sem=rs_recv.at[src], device_id={'feat': src}, device_id_type=MESH)

    def send_products(before):
        for d in far_first:
            z = chip_at(d)
            before(z, d)
            u = product(z)
            if d:
                usend[2 * z] = u[:, :LANES]
                usend[2 * z + 1] = u[:, LANES:]
                rs_copy(2 * z + core).start()
                rs_copy(2 * z + 1 - core).start()
            else:
                usend[2 * z] = u[:, :LANES]
                usend[2 * z + 1] = u[:, LANES:]
                rs_copy(partner).start()

    def summed():
        total = usend[me].astype(F32)
        for d in near_first:
            z = chip_at(d)
            for src in ((partner,) if d == 0 else (2 * z + core, 2 * z + 1 - core)):
                rs_arrival(src).wait_recv()
                total = total + rs[src].astype(F32)
        return total

    def finish_sends():
        for d in far_first:
            z = chip_at(d)
            for dst in ((partner,) if d == 0 else (2 * z + core, 2 * z + 1 - core)):
                rs_copy(dst).wait_send()

    def gather_copy(buf, slot, dst, send_sem, recv_sem):
        return pltpu.make_async_remote_copy(src_ref=buf.at[slot], dst_ref=buf.at[slot], send_sem=send_sem, recv_sem=recv_sem.at[slot], device_id={'feat': dst}, device_id_type=MESH)

    def gather(buf, send_sem, recv_sem, fwd_sem, use):
        for d in far_first:
            dst = partner if d == 0 else 2 * chip_at(d) + core
            gather_copy(buf, me, dst, send_sem.at[d], recv_sem).start()
        use(me)
        gather_copy(buf, partner, partner, send_sem.at[0], recv_sem).wait_recv()
        use(partner)

        def same(d):
            slot = 2 * chip_at(d) + core
            gather_copy(buf, slot, slot, send_sem.at[d], recv_sem).wait_recv()
            gather_copy(buf, slot, partner, fwd_sem.at[d], recv_sem).start()
            use(slot)

        def other(d):
            slot = 2 * chip_at(d) + 1 - core
            gather_copy(buf, slot, partner, fwd_sem.at[d], recv_sem).wait_recv()
            use(slot)

        half = chips // 2
        groups = [[k, chips - k] for k in range(1, half)] + [[half]]
        for i, pair in enumerate(groups):
            for d in pair:
                same(d)
            if i:
                for d in groups[i - 1]:
                    other(d)
        for d in groups[-1]:
            other(d)
        for d in far_first:
            dst = partner if d == 0 else 2 * chip_at(d) + core
            gather_copy(buf, me, dst, send_sem.at[d], recv_sem).wait_send()
            if d:
                gather_copy(buf, 2 * chip_at(d) + core, partner, fwd_sem.at[d], recv_sem).wait_send()

    eta = jnp.broadcast_to(eta_ref[...], (SUB, width))
    for t in range(targets):
        wbuf[pl.ds(t * SUB, SUB), :] = jnp.broadcast_to(w0_ref[pl.ds(t, 1), :], (SUB, width))
    fill_lhs(wbuf[...])
    pl.semaphore_wait(barrier, group - 1)
    send_products(lambda z, d: x_copy(z, d).wait())
    y_copy.wait()
    for s in range(blocks):
        rbuf[pl.ds(s, targets, stride=SUB), :] = yv[:, s * LANES:(s + 1) * LANES]
    rbuf[...] = rbuf[...] - summed()
    finish_sends()

    eta_all = jnp.concatenate([eta] * targets, axis=0)

    def sweep(_, carry):
        ag[me] = rbuf[...].astype(BF16)
        acc = []

        def use(slot):
            chunk = ag[slot]
            lhs = jnp.concatenate([pick(chunk, s) for s in range(blocks)], axis=1)
            part = jnp.dot(lhs, xv[pl.ds(pl.multiple_of(slot * own, own), own), :], preferred_element_type=F32)
            acc.append(part if not acc else acc[-1] + part)

        gather(ag, ag_send, ag_recv, fwd_send, use)
        gsum = acc[-1]
        per_target = [jnp.broadcast_to(jnp.sum(gsum[t * SUB:(t + 1) * SUB], axis=0, keepdims=True), (SUB, width)) for t in range(targets)]
        gradient = jnp.concatenate(per_target, axis=0) / samples
        weights = wbuf[...]
        stepped = weights + eta_all * gradient
        limit = eta_all * lasso_weight
        shrunk = jnp.maximum(stepped - limit, 0.0) + jnp.minimum(stepped + limit, 0.0)
        change = shrunk - weights
        wbuf[...] = weights + COMBINE_WEIGHT * change
        fill_lhs(change)
        send_products(lambda z, d: None)
        rbuf[...] = rbuf[...] - COMBINE_WEIGHT * summed()
        finish_sends()
        return carry

    lax.fori_loop(0, SWEEPS, sweep, 0)

    for t in range(targets):
        wt_ref[pl.ds(t, 1), :] = wbuf[pl.ds(t * SUB, 1), :]
    agf[me] = rbuf[...]

    def unpack(slot):
        for s in range(blocks):
            rt_ref[:, pl.ds(pl.multiple_of(slot * own, own) + s * LANES, LANES)] = agf[slot, pl.ds(s, targets, stride=SUB), :]

    gather(agf, fin_send, fin_recv, ffwd_send, unpack)


def solution(mesh):
    group = mesh.shape['feat']

    def local_run(x_local, coef_local, targets_local, step_local):
        samples, width = x_local.shape
        targets = coef_local.shape[1]
        lasso_weight = 0.3 * group / (width * group) ** 0.5
        rows = targets * SUB
        chips = group // 2
        dma = pltpu.SemaphoreType.DMA
        wt, rt = pl.pallas_call(
            functools.partial(kernel, group, lasso_weight),
            out_shape=(jax.ShapeDtypeStruct((targets, width), F32), jax.ShapeDtypeStruct((targets, samples), F32)),
            in_specs=[pl.BlockSpec(memory_space=pl.ANY), pl.BlockSpec(memory_space=pltpu.VMEM), pl.BlockSpec(memory_space=pl.ANY), pl.BlockSpec(memory_space=pltpu.VMEM)],
            out_specs=(pl.BlockSpec(memory_space=pltpu.VMEM), pl.BlockSpec(memory_space=pltpu.VMEM)),
            scratch_shapes=[
                pltpu.VMEM((samples, width), BF16),
                pltpu.VMEM((targets, samples // group), F32),
                pltpu.VMEM((SUB, rows, width), BF16),
                pltpu.VMEM((group, rows, LANES), BF16),
                pltpu.VMEM((group, rows, LANES), BF16),
                pltpu.VMEM((group, rows, LANES), BF16),
                pltpu.VMEM((group, rows, LANES), F32),
                pltpu.VMEM((rows, LANES), F32),
                pltpu.VMEM((rows, width), F32),
                dma((chips,)),
                dma,
                dma((group,)),
                dma((group,)),
                dma((chips,)),
                dma((group,)),
                dma((chips,)),
                dma((chips,)),
                dma((group,)),
                dma((chips,)),
            ],
            compiler_params=pltpu.CompilerParams(collective_id=0, has_side_effects=True),
            name='lasso',
        )(x_local, coef_local.T, targets_local.T, step_local[None, :])
        return wt.T, rt.T

    return jax.shard_map(local_run, mesh=mesh, in_specs=(P('prob', 'feat'), P(('prob', 'feat'), None), P('prob', None), P(('prob', 'feat'))), out_specs=(P(('prob', 'feat'), None), P('prob', None)), check_vma=False)
```

```python
import functools

import jax
import jax.numpy as jnp
from jax import lax
from jax.experimental import pallas as pl
from jax.experimental.pallas import tpu as pltpu
from jax.sharding import PartitionSpec as P

SWEEPS = 6
COMBINE_WEIGHT = 0.8
LANES = 128
SUB = 8
MESH = pl.DeviceIdType.MESH
F32 = jnp.float32
BF16 = jnp.bfloat16


def ring_order(chips):
    order = [chips // 2]
    for d in range(chips // 2 - 1, 0, -1):
        order += [d, chips - d]
    return order + [0]


def kernel(group, chains, lasso_weight, x_hbm, w0_ref, y_hbm, eta_ref, wt_ref, rt_ref,
           xv, xt, yv, lbuf, usend, rs, ag, agf, rbuf, wbuf,
           x_sem, y_sem, rs_send, rs_recv, ag_send, ag_recv, fwd_send, fin_send, fin_recv, ffwd_send):
    chips = group // 2
    samples, width = xv.shape
    own = samples // group
    blocks = own // LANES
    targets = w0_ref.shape[0]
    part_targets = targets // chains
    rows = part_targets * SUB
    me = lax.axis_index('feat')
    chip = me // 2
    core = me % 2
    partner = chip * 2 + (1 - core)
    far_first = ring_order(chips)
    near_first = far_first[::-1]
    half = chips // 2

    def chip_at(d):
        return (chip + d) % chips

    def peers(d):
        z = chip_at(d)
        return (partner,) if d == 0 else (2 * z + core, 2 * z + 1 - core)

    barrier = pltpu.get_barrier_semaphore()
    for k in range(1, group):
        pl.semaphore_signal(barrier, inc=1, device_id={'feat': (me + k) % group}, device_id_type=MESH)

    def x_copy(z, d):
        part = pl.ds(pl.multiple_of(z * (2 * own), 2 * own), 2 * own)
        return pltpu.make_async_copy(x_hbm.at[part, :], xv.at[part, :], x_sem.at[d])

    y_copy = pltpu.make_async_copy(y_hbm.at[:, pl.ds(pl.multiple_of(me * own, own), own)], yv, y_sem)
    for d in far_first:
        x_copy(chip_at(d), d).start()
    y_copy.start()

    row_id = lax.broadcasted_iota(jnp.int32, (rows, LANES), 0)
    sub_masks = [(row_id % SUB) == s for s in range(SUB)]

    def pick(value, s):
        wide = [jnp.where(sub_masks[s], value[:, i * LANES:(i + 1) * LANES], jnp.zeros((), value.dtype)) for i in range(value.shape[1] // LANES)]
        return wide[0] if len(wide) == 1 else jnp.concatenate(wide, axis=1)

    def fill_lhs(c, values):
        for s in range(SUB):
            lbuf[c, :, s * width:(s + 1) * width] = pick(values, s).astype(BF16)

    def first_product(z):
        base = pl.multiple_of(z * (2 * own), 2 * own)
        lhs = jnp.concatenate([lbuf[c] for c in range(chains)], axis=0)
        for h in range(2):
            total = None
            for s in range(blocks):
                x_part = xv[pl.ds(base + h * own + s * LANES, LANES), :]
                part = lax.dot_general(lhs[:, s * width:(s + 1) * width], x_part, (((1,), (1,)), ((), ())), preferred_element_type=F32)
                total = part if total is None else total + part
            u = total.astype(BF16)
            for c in range(chains):
                usend[c, 2 * z + h] = u[c * rows:(c + 1) * rows]

    def transpose_x(z):
        base = pl.multiple_of(z * (2 * own), 2 * own)
        for s in range(blocks):
            for h in range(2):
                x_part = xv[pl.ds(base + h * own + s * LANES, LANES), :]
                xt[pl.ds(base + s * width, width), h * LANES:(h + 1) * LANES] = x_part.T

    def product(c, z):
        base = pl.multiple_of(z * (2 * own), 2 * own)
        for h in range(2):
            u = jnp.dot(lbuf[c], xt[pl.ds(base, blocks * width), h * LANES:(h + 1) * LANES], preferred_element_type=F32)
            usend[c, 2 * z + h] = u.astype(BF16)

    def rs_copy(c, dst):
        return pltpu.make_async_remote_copy(src_ref=usend.at[c, dst], dst_ref=rs.at[c, me], send_sem=rs_send.at[c, dst], recv_sem=rs_recv.at[c, me], device_id={'feat': dst}, device_id_type=MESH)

    def rs_arrival(c, src):
        return pltpu.make_async_remote_copy(src_ref=usend.at[c, src], dst_ref=rs.at[c, src], send_sem=rs_send.at[c, src], recv_sem=rs_recv.at[c, src], device_id={'feat': src}, device_id_type=MESH)

    def send_products(c, compute):
        for d in far_first:
            if compute:
                product(c, chip_at(d))
            for dst in peers(d):
                rs_copy(c, dst).start()

    def summed(c):
        total = usend[c, me].astype(F32)
        for d in near_first:
            for src in peers(d):
                rs_arrival(c, src).wait_recv()
                total = total + rs[c, src].astype(F32)
        for d in far_first:
            for dst in peers(d):
                rs_copy(c, dst).wait_send()
        return total

    def gather_copy(buf, c, slot, dst, send_sem, recv_sem):
        return pltpu.make_async_remote_copy(src_ref=buf.at[c, slot], dst_ref=buf.at[c, slot], send_sem=send_sem, recv_sem=recv_sem.at[c, slot], device_id={'feat': dst}, device_id_type=MESH)

    def same_core(d):
        return partner if d == 0 else 2 * chip_at(d) + core

    def gather_start(buf, c, send_sem, recv_sem):
        for d in far_first:
            gather_copy(buf, c, me, same_core(d), send_sem.at[c, d], recv_sem).start()

    def gather_finish(buf, c, send_sem, recv_sem, fwd_sem, use):
        use(me)
        gather_copy(buf, c, partner, partner, send_sem.at[c, 0], recv_sem).wait_recv()
        use(partner)

        def same(d):
            slot = same_core(d)
            gather_copy(buf, c, slot, slot, send_sem.at[c, d], recv_sem).wait_recv()
            gather_copy(buf, c, slot, partner, fwd_sem.at[c, d], recv_sem).start()
            use(slot)

        def other(d):
            slot = 2 * chip_at(d) + 1 - core
            gather_copy(buf, c, slot, partner, fwd_sem.at[c, d], recv_sem).wait_recv()
            use(slot)

        groups = [[k, chips - k] for k in range(1, half)] + [[half]]
        for i, pair in enumerate(groups):
            for d in pair:
                same(d)
            if i:
                for d in groups[i - 1]:
                    other(d)
        for d in groups[-1]:
            other(d)
        for d in far_first:
            gather_copy(buf, c, me, same_core(d), send_sem.at[c, d], recv_sem).wait_send()
            if d:
                gather_copy(buf, c, same_core(d), partner, fwd_sem.at[c, d], recv_sem).wait_send()

    eta = jnp.broadcast_to(eta_ref[...], (rows, width))
    limit = eta * lasso_weight
    for c in range(chains):
        first = c * part_targets
        for t in range(part_targets):
            wbuf[c, t * SUB:(t + 1) * SUB, :] = jnp.broadcast_to(w0_ref[first + t:first + t + 1, :], (SUB, width))
        fill_lhs(c, wbuf[c])
    for d in far_first:
        x_copy(chip_at(d), d).wait()
        first_product(chip_at(d))
    pl.semaphore_wait(barrier, group - 1)
    for c in range(chains):
        send_products(c, False)

    def transpose_step(z, carry):
        transpose_x(z)
        return carry

    lax.fori_loop(0, chips, transpose_step, 0)
    y_copy.wait()
    for c in range(chains):
        first = c * part_targets
        for s in range(blocks):
            rbuf[c, pl.ds(s, part_targets, stride=SUB), :] = yv[first:first + part_targets, s * LANES:(s + 1) * LANES]
        rbuf[c] = rbuf[c] - summed(c)
        ag[c, me] = rbuf[c].astype(BF16)
        gather_start(ag, c, ag_send, ag_recv)

    def update(c):
        acc = [None, None]

        def use(slot):
            chunk = ag[c, slot]
            lhs = jnp.concatenate([pick(chunk, s) for s in range(blocks)], axis=1)
            for h in range(2):
                part = jnp.dot(lhs, xv[pl.ds(pl.multiple_of(slot * own, own), own), h * LANES:(h + 1) * LANES], preferred_element_type=F32)
                acc[h] = part if acc[h] is None else acc[h] + part

        gather_finish(ag, c, ag_send, ag_recv, fwd_send, use)
        gsum = jnp.concatenate(acc, axis=1)
        per_target = [jnp.broadcast_to(jnp.sum(gsum[t * SUB:(t + 1) * SUB], axis=0, keepdims=True), (SUB, width)) for t in range(part_targets)]
        gradient = jnp.concatenate(per_target, axis=0) / samples
        weights = wbuf[c]
        stepped = weights + eta * gradient
        shrunk = jnp.maximum(stepped - limit, 0.0) + jnp.minimum(stepped + limit, 0.0)
        change = shrunk - weights
        wbuf[c] = weights + COMBINE_WEIGHT * change
        fill_lhs(c, change)
        send_products(c, True)

    def advance(c):
        rbuf[c] = rbuf[c] - COMBINE_WEIGHT * summed(c)

    def sweep(_, carry):
        for c in range(chains):
            update(c)
        for c in range(chains):
            advance(c)
            ag[c, me] = rbuf[c].astype(BF16)
            gather_start(ag, c, ag_send, ag_recv)
        return carry

    lax.fori_loop(0, SWEEPS - 1, sweep, 0)
    for c in range(chains):
        update(c)
    for c in range(chains):
        advance(c)
        agf[c, me] = rbuf[c]
        gather_start(agf, c, fin_send, fin_recv)
    for c in range(chains):
        first = c * part_targets
        for t in range(part_targets):
            wt_ref[first + t:first + t + 1, :] = wbuf[c, t * SUB:t * SUB + 1, :]

        def unpack(slot):
            for s in range(blocks):
                rt_ref[first:first + part_targets, pl.ds(pl.multiple_of(slot * own, own) + s * LANES, LANES)] = agf[c, slot, pl.ds(s, part_targets, stride=SUB), :]

        gather_finish(agf, c, fin_send, fin_recv, ffwd_send, unpack)


def solution(mesh):
    group = mesh.shape['feat']

    def local_run(x_local, coef_local, targets_local, step_local):
        samples, width = x_local.shape
        targets = coef_local.shape[1]
        lasso_weight = 0.3 * group / (width * group) ** 0.5
        chains = 2
        rows = targets // chains * SUB
        chips = group // 2
        dma = pltpu.SemaphoreType.DMA
        wt, rt = pl.pallas_call(
            functools.partial(kernel, group, chains, lasso_weight),
            out_shape=(jax.ShapeDtypeStruct((targets, width), F32), jax.ShapeDtypeStruct((targets, samples), F32)),
            in_specs=[pl.BlockSpec(memory_space=pl.ANY), pl.BlockSpec(memory_space=pltpu.VMEM), pl.BlockSpec(memory_space=pl.ANY), pl.BlockSpec(memory_space=pltpu.VMEM)],
            out_specs=(pl.BlockSpec(memory_space=pltpu.VMEM), pl.BlockSpec(memory_space=pltpu.VMEM)),
            scratch_shapes=[
                pltpu.VMEM((samples, width), BF16),
                pltpu.VMEM((samples, width), BF16),
                pltpu.VMEM((targets, samples // group), F32),
                pltpu.VMEM((chains, rows, SUB * width), BF16),
                pltpu.VMEM((chains, group, rows, LANES), BF16),
                pltpu.VMEM((chains, group, rows, LANES), BF16),
                pltpu.VMEM((chains, group, rows, LANES), BF16),
                pltpu.VMEM((chains, group, rows, LANES), F32),
                pltpu.VMEM((chains, rows, LANES), F32),
                pltpu.VMEM((chains, rows, width), F32),
                dma((chips,)),
                dma,
                dma((chains, group)),
                dma((chains, group)),
                dma((chains, chips)),
                dma((chains, group)),
                dma((chains, chips)),
                dma((chains, chips)),
                dma((chains, group)),
                dma((chains, chips)),
            ],
            compiler_params=pltpu.CompilerParams(collective_id=0, has_side_effects=True),
            name='lasso',
        )(x_local, coef_local.T, targets_local.T, step_local[None, :])
        return wt.T, rt.T

    return jax.shard_map(local_run, mesh=mesh, in_specs=(P('prob', 'feat'), P(('prob', 'feat'), None), P('prob', None), P(('prob', 'feat'))), out_specs=(P(('prob', 'feat'), None), P('prob', None)), check_vma=False)
```

```python
import functools

import jax
import jax.numpy as jnp
from jax import lax
from jax.experimental import pallas as pl
from jax.experimental.pallas import tpu as pltpu
from jax.sharding import PartitionSpec as P

SWEEPS = 6
COMBINE_WEIGHT = 0.8
LANES = 128
SUB = 8
MESH = pl.DeviceIdType.MESH
F32 = jnp.float32
BF16 = jnp.bfloat16


def ring_order(chips):
    order = [chips // 2]
    for d in range(chips // 2 - 1, 0, -1):
        order += [d, chips - d]
    return order + [0]


def kernel(group, chains, lasso_weight, x_hbm, w0_ref, y_hbm, eta_ref, wt_ref, rt_ref,
           xv, xt, yv, lbuf0, lbuf, usend, rs, ag, agf, rbuf, wbuf,
           x_sem, y_sem, rs_send, rs_recv, ag_send, ag_recv, fwd_send, fin_send, fin_recv, ffwd_send):
    chips = group // 2
    samples, width = xv.shape
    own = samples // group
    blocks = own // LANES
    targets = w0_ref.shape[0]
    part_targets = targets // chains
    rows = part_targets * SUB
    me = lax.axis_index('feat')
    chip = me // 2
    core = me % 2
    partner = chip * 2 + (1 - core)
    far_first = ring_order(chips)
    near_first = far_first[::-1]
    half = chips // 2

    def chip_at(d):
        return (chip + d) % chips

    def peers(d):
        z = chip_at(d)
        return (partner,) if d == 0 else (2 * z + core, 2 * z + 1 - core)

    barrier = pltpu.get_barrier_semaphore()
    for k in range(1, group):
        pl.semaphore_signal(barrier, inc=1, device_id={'feat': (me + k) % group}, device_id_type=MESH)

    def x_copy(z, d):
        part = pl.ds(pl.multiple_of(z * (2 * own), 2 * own), 2 * own)
        return pltpu.make_async_copy(x_hbm.at[part, :], xv.at[part, :], x_sem.at[d])

    y_copy = pltpu.make_async_copy(y_hbm.at[:, pl.ds(pl.multiple_of(me * own, own), own)], yv, y_sem)
    for d in far_first:
        x_copy(chip_at(d), d).start()
    y_copy.start()

    row_id = lax.broadcasted_iota(jnp.int32, (targets * SUB, LANES), 0)
    sub_masks = [(row_id % SUB) == s for s in range(SUB)]

    def pick(value, s):
        mask = sub_masks[s][:value.shape[0]]
        wide = [jnp.where(mask, value[:, i * LANES:(i + 1) * LANES], jnp.zeros((), value.dtype)) for i in range(value.shape[1] // LANES)]
        return wide[0] if len(wide) == 1 else jnp.concatenate(wide, axis=1)

    def fill_lhs(put, values):
        for s in range(SUB):
            put(s, pick(values if s < SUB // 2 else -values, s).astype(BF16))

    def store_product(c, z, u):
        u = u.astype(BF16)
        usend[c, 2 * z] = u[:, :LANES]
        usend[c, 2 * z + 1] = u[:, LANES:]

    def first_product(z):
        base = pl.multiple_of(z * (2 * own), 2 * own)
        sums = []
        for side in range(2):
            total = None
            for s in range(side * blocks // 2, (side + 1) * blocks // 2):
                x_part = jnp.concatenate([xv[pl.ds(base + h * own + s * LANES, LANES), :] for h in range(2)], axis=0)
                part = lax.dot_general(lbuf0[:, s * width:(s + 1) * width], x_part, (((1,), (1,)), ((), ())), preferred_element_type=F32)
                total = part if total is None else total + part
            sums.append(total)
        u = sums[0] - sums[1]
        for c in range(chains):
            store_product(c, z, u[c * rows:(c + 1) * rows])

    def product(c, z):
        base = pl.multiple_of(z * (2 * own), 2 * own)
        depth = blocks * width // 2
        sums = [jnp.dot(lbuf[c, :, side * depth:(side + 1) * depth], xt[pl.ds(base + side * depth, depth), :], preferred_element_type=F32) for side in range(2)]
        store_product(c, z, sums[0] - sums[1])

    def rs_copy(c, dst):
        return pltpu.make_async_remote_copy(src_ref=usend.at[c, dst], dst_ref=rs.at[c, me], send_sem=rs_send.at[c, dst], recv_sem=rs_recv.at[c, me], device_id={'feat': dst}, device_id_type=MESH)

    def rs_arrival(c, src):
        return pltpu.make_async_remote_copy(src_ref=usend.at[c, src], dst_ref=rs.at[c, src], send_sem=rs_send.at[c, src], recv_sem=rs_recv.at[c, src], device_id={'feat': src}, device_id_type=MESH)

    def send_products(c, compute):
        for d in far_first:
            if compute:
                product(c, chip_at(d))
            for dst in peers(d):
                rs_copy(c, dst).start()

    def summed(c):
        total = usend[c, me].astype(F32)
        for d in near_first:
            for src in peers(d):
                rs_arrival(c, src).wait_recv()
                total = total + rs[c, src].astype(F32)
        for d in far_first:
            for dst in peers(d):
                rs_copy(c, dst).wait_send()
        return total

    def gather_copy(buf, c, slot, dst, send_sem, recv_sem):
        return pltpu.make_async_remote_copy(src_ref=buf.at[c, slot], dst_ref=buf.at[c, slot], send_sem=send_sem, recv_sem=recv_sem.at[c, slot], device_id={'feat': dst}, device_id_type=MESH)

    def same_core(d):
        return partner if d == 0 else 2 * chip_at(d) + core

    def gather_start(buf, c, send_sem, recv_sem):
        for d in far_first:
            gather_copy(buf, c, me, same_core(d), send_sem.at[c, d], recv_sem).start()

    def gather_steps(buf, c, send_sem, recv_sem, fwd_sem):
        def from_partner():
            gather_copy(buf, c, partner, partner, send_sem.at[c, 0], recv_sem).wait_recv()

        def same(d):
            slot = same_core(d)

            def arrive():
                gather_copy(buf, c, slot, slot, send_sem.at[c, d], recv_sem).wait_recv()
                gather_copy(buf, c, slot, partner, fwd_sem.at[c, d], recv_sem).start()

            return arrive, slot

        def other(d):
            slot = 2 * chip_at(d) + 1 - core
            return gather_copy(buf, c, slot, partner, fwd_sem.at[c, d], recv_sem).wait_recv, slot

        steps = [(lambda: None, me), (from_partner, partner)]
        groups = [[k, chips - k] for k in range(1, half)] + [[half]]
        for i, pair in enumerate(groups):
            steps += [same(d) for d in pair]
            if i:
                steps += [other(d) for d in groups[i - 1]]
        return steps + [other(d) for d in groups[-1]]

    def gather_drain(buf, c, send_sem, recv_sem, fwd_sem):
        for d in far_first:
            gather_copy(buf, c, me, same_core(d), send_sem.at[c, d], recv_sem).wait_send()
            if d:
                gather_copy(buf, c, same_core(d), partner, fwd_sem.at[c, d], recv_sem).wait_send()

    eta = jnp.broadcast_to(eta_ref[...], (rows, width))
    limit = eta * lasso_weight

    def put0(s, value):
        lbuf0[:, s * width:(s + 1) * width] = value

    for c in range(chains):
        base = c * part_targets
        for t in range(part_targets):
            wbuf[c, t * SUB:(t + 1) * SUB, :] = jnp.broadcast_to(w0_ref[base + t:base + t + 1, :], (SUB, width))
    fill_lhs(put0, jnp.concatenate([wbuf[c] for c in range(chains)], axis=0))
    for d in far_first:
        x_copy(chip_at(d), d).wait()
        first_product(chip_at(d))
    pl.semaphore_wait(barrier, group - 1)
    for c in range(chains):
        send_products(c, False)

    def transpose_step(z, carry):
        base = pl.multiple_of(z * (2 * own), 2 * own)
        for s in range(blocks):
            for h in range(2):
                x_part = xv[pl.ds(base + h * own + s * LANES, LANES), :]
                xt[pl.ds(base + s * width, width), h * LANES:(h + 1) * LANES] = x_part.T
        return carry

    lax.fori_loop(0, chips, transpose_step, 0)
    y_copy.wait()
    for c in range(chains):
        base = c * part_targets
        for s in range(blocks):
            rbuf[c, pl.ds(s, part_targets, stride=SUB), :] = yv[base:base + part_targets, s * LANES:(s + 1) * LANES]

    def start_gather(c):
        ag[c, me] = rbuf[c].astype(BF16)
        gather_start(ag, c, ag_send, ag_recv)

    def gradient_pair(c):
        acc = [None, None]
        depth = own // 2
        side_blocks = blocks // 2
        for arrive, slot in gather_steps(ag, c, ag_send, ag_recv, fwd_send):
            arrive()
            chunk = ag[c, slot]
            for side in range(2):
                lhs = jnp.concatenate([pick(chunk, side * side_blocks + i) for i in range(side_blocks)], axis=1)
                part = jnp.dot(lhs, xv[pl.ds(pl.multiple_of(slot * own, own) + side * depth, depth), :], preferred_element_type=F32)
                acc[side] = part if acc[side] is None else acc[side] + part
        gather_drain(ag, c, ag_send, ag_recv, fwd_send)
        return acc

    def update(c, acc):
        weights = wbuf[c]
        scaled = acc[0] / samples + acc[1] / samples
        gradient = jnp.concatenate([jnp.broadcast_to(jnp.sum(scaled[t * SUB:(t + 1) * SUB], axis=0, keepdims=True), (SUB, width)) for t in range(part_targets)], axis=0)
        stepped = weights + eta * gradient
        shrunk = jnp.maximum(stepped - limit, 0.0) + jnp.minimum(stepped + limit, 0.0)
        change = shrunk - weights
        wbuf[c] = weights + COMBINE_WEIGHT * change

        def put(s, value):
            lbuf[c, :, s * width:(s + 1) * width] = value

        fill_lhs(put, change)
        send_products(c, True)

    def advance(c):
        rbuf[c] = rbuf[c] - COMBINE_WEIGHT * summed(c)

    def finish_start(c):
        agf[c, me] = rbuf[c]
        gather_start(agf, c, fin_send, fin_recv)

    def finish_rest(c):
        base = c * part_targets
        for t in range(part_targets):
            wt_ref[base + t:base + t + 1, :] = wbuf[c, t * SUB:t * SUB + 1, :]
        for arrive, slot in gather_steps(agf, c, fin_send, fin_recv, ffwd_send):
            arrive()
            for s in range(blocks):
                rt_ref[base:base + part_targets, pl.ds(pl.multiple_of(slot * own, own) + s * LANES, LANES)] = agf[c, slot, pl.ds(s, part_targets, stride=SUB), :]
        gather_drain(agf, c, fin_send, fin_recv, ffwd_send)

    for c in range(chains):
        rbuf[c] = rbuf[c] - summed(c)
        start_gather(c)
    update(0, gradient_pair(0))

    def sweep(_, carry):
        acc = gradient_pair(1)
        advance(0)
        start_gather(0)
        update(1, acc)
        acc = gradient_pair(0)
        advance(1)
        start_gather(1)
        update(0, acc)
        return carry

    lax.fori_loop(0, SWEEPS - 1, sweep, 0)
    acc = gradient_pair(1)
    advance(0)
    finish_start(0)
    update(1, acc)
    finish_rest(0)
    advance(1)
    finish_start(1)
    finish_rest(1)


def solution(mesh):
    group = mesh.shape['feat']

    def local_run(x_local, coef_local, targets_local, step_local):
        samples, width = x_local.shape
        targets = coef_local.shape[1]
        lasso_weight = 0.3 * group / (width * group) ** 0.5
        chains = 2
        rows = targets // chains * SUB
        chips = group // 2
        dma = pltpu.SemaphoreType.DMA
        wt, rt = pl.pallas_call(
            functools.partial(kernel, group, chains, lasso_weight),
            out_shape=(jax.ShapeDtypeStruct((targets, width), F32), jax.ShapeDtypeStruct((targets, samples), F32)),
            in_specs=[pl.BlockSpec(memory_space=pl.ANY), pl.BlockSpec(memory_space=pltpu.VMEM), pl.BlockSpec(memory_space=pl.ANY), pl.BlockSpec(memory_space=pltpu.VMEM)],
            out_specs=(pl.BlockSpec(memory_space=pltpu.VMEM), pl.BlockSpec(memory_space=pltpu.VMEM)),
            scratch_shapes=[
                pltpu.VMEM((samples, width), BF16),
                pltpu.VMEM((samples, width), BF16),
                pltpu.VMEM((targets, samples // group), F32),
                pltpu.VMEM((targets * SUB, SUB * width), BF16),
                pltpu.VMEM((chains, rows, SUB * width), BF16),
                pltpu.VMEM((chains, group, rows, LANES), BF16),
                pltpu.VMEM((chains, group, rows, LANES), BF16),
                pltpu.VMEM((chains, group, rows, LANES), BF16),
                pltpu.VMEM((chains, group, rows, LANES), F32),
                pltpu.VMEM((chains, rows, LANES), F32),
                pltpu.VMEM((chains, rows, width), F32),
                dma((chips,)),
                dma,
                dma((chains, group)),
                dma((chains, group)),
                dma((chains, chips)),
                dma((chains, group)),
                dma((chains, chips)),
                dma((chains, chips)),
                dma((chains, group)),
                dma((chains, chips)),
            ],
            compiler_params=pltpu.CompilerParams(collective_id=0, has_side_effects=True),
            name='lasso',
        )(x_local, coef_local.T, targets_local.T, step_local[None, :])
        return wt.T, rt.T

    return jax.shard_map(local_run, mesh=mesh, in_specs=(P('prob', 'feat'), P(('prob', 'feat'), None), P('prob', None), P(('prob', 'feat'))), out_specs=(P(('prob', 'feat'), None), P('prob', None)), check_vma=False)
```
